32 devices in a mesh: data: 1 (over z), ep: 32 (over y, x, core).
Axes of the slice: x: 4, y: 4, z: 1, core: 2. Of those that a mesh axis runs over, the one named last changes fastest.
The devices are a block of a 4x4x8 slice.
Arguments:
- x_in: bfloat16 [32, 2048, 1024], P(('data', 'ep'))
- w_query: bfloat16 [1024, 16, 64], P('ep')
- w_keyval: bfloat16 [1024, 16, 64], P('ep')
- w_out: bfloat16 [1024, 1024], P('ep')
- attn_gain: bfloat16 [1024], replicated
- moe_gain: bfloat16 [1024], replicated
- w_gate: bfloat16 [32, 1024, 512], P(None, 'ep')
- w_up: bfloat16 [32, 1024, 512], P(None, 'ep')
- w_down: bfloat16 [32, 512, 1024], P(None, None, 'ep')
- expert_ids: int32 [32, 2048, 8], P(('data', 'ep'))
- slot_ids: int32 [32, 2048, 8], P(('data', 'ep'))
- fill_counts: int32 [32, 32], P(('data', 'ep'))
- route_weight: bfloat16 [32, 2048, 8], P(('data', 'ep'))
Outputs:
- output: bfloat16 [32, 2048, 1024], P(('data', 'ep'))
All inputs are finite; a program needn't handle non-finite values.
Results may differ from the reference program's by a relative error of at most 0.02.
Values are sent between devices in bfloat16 or wider.
A program may use at most 768 MiB of HBM per device.

```python
import jax
import jax.numpy as jnp
from jax import lax

D = 1024
FF = 512
EXPERTS = 32
TOP = 8
HEADS = 16
KV_HEADS = 8
HEAD_DIM = 64
GROUP = 32
BATCH_DEV = 1
SEQ = 2048

TOKENS_DEV = BATCH_DEV * SEQ
CAPACITY = 2 * TOKENS_DEV * TOP // EXPERTS
BATCH = GROUP * BATCH_DEV


def expert_stack(stack_key, rows, cols, scale):
    def one_expert(expert_key):
        return (jax.random.normal(expert_key, (rows, cols), jnp.float32) * scale).astype(jnp.bfloat16)
    return lax.map(one_expert, jax.random.split(stack_key, EXPERTS))


def draw_routing(route_key):
    bias_key, hot_key, noise_key, cap_key = jax.random.split(route_key, 4)
    expert_bias = jax.random.randint(bias_key, (EXPERTS,), 0, EXPERTS)
    hot_expert = jax.random.randint(hot_key, (), 0, EXPERTS)
    is_hot = jnp.arange(EXPERTS) == hot_expert
    noise = jax.random.randint(noise_key, (GROUP, TOKENS_DEV, EXPERTS), 0, 2 * EXPERTS)
    scores = (expert_bias + jnp.where(is_hot, 4 * EXPERTS, 0) + noise) * EXPERTS + jnp.arange(EXPERTS)
    picked = lax.top_k(scores, TOP)[1]
    onehot = (picked.reshape(GROUP, TOKENS_DEV * TOP, 1) == jnp.arange(EXPERTS)).astype(jnp.int32)
    prior_hits = jnp.cumsum(onehot, axis=1) - onehot
    slot_ids = jnp.sum(prior_hits * onehot, axis=-1)
    demand = jnp.sum(onehot, axis=1)
    cap_draw = jax.random.randint(cap_key, (GROUP, EXPERTS), CAPACITY // 2, CAPACITY + 1)
    fill_counts = jnp.minimum(demand, jnp.where(is_hot, CAPACITY, cap_draw))
    return (picked.reshape(BATCH, SEQ, TOP).astype(jnp.int32), slot_ids.reshape(BATCH, SEQ, TOP).astype(jnp.int32), fill_counts.astype(jnp.int32))


def setup_inputs(seed: int = 0, part: int = 0) -> dict:
    root_key = jax.random.key(seed)
    weight_keys = jax.random.split(root_key, 8)
    part_keys = jax.random.split(jax.random.fold_in(root_key, part), 3)
    x_in = jax.random.normal(part_keys[0], (BATCH, SEQ, D), jnp.float32).astype(jnp.bfloat16)
    w_query = (jax.random.normal(weight_keys[0], (D, HEADS, HEAD_DIM), jnp.float32) * (2.0 * D ** -0.5)).astype(jnp.bfloat16)
    w_keyval = (jax.random.normal(weight_keys[1], (D, 2 * KV_HEADS, HEAD_DIM), jnp.float32) * (2.0 * D ** -0.5)).astype(jnp.bfloat16)
    w_out = (jax.random.normal(weight_keys[2], (HEADS * HEAD_DIM, D), jnp.float32) * (HEADS * HEAD_DIM) ** -0.5).astype(jnp.bfloat16)
    attn_gain = jax.random.uniform(weight_keys[3], (D,), jnp.float32, 0.5, 1.5).astype(jnp.bfloat16)
    moe_gain = jax.random.uniform(weight_keys[4], (D,), jnp.float32, 0.5, 1.5).astype(jnp.bfloat16)
    w_gate = expert_stack(weight_keys[5], D, FF, D ** -0.5)
    w_up = expert_stack(weight_keys[6], D, FF, D ** -0.5)
    w_down = expert_stack(weight_keys[7], FF, D, 2.0 * FF ** -0.5)
    expert_ids, slot_ids, fill_counts = draw_routing(part_keys[1])
    route_weight = jax.random.uniform(part_keys[2], (BATCH, SEQ, TOP), jnp.float32, 0.25, 1.0).astype(jnp.bfloat16)
    return {'x_in': x_in, 'w_query': w_query, 'w_keyval': w_keyval, 'w_out': w_out, 'attn_gain': attn_gain, 'moe_gain': moe_gain, 'w_gate': w_gate, 'w_up': w_up, 'w_down': w_down, 'expert_ids': expert_ids, 'slot_ids': slot_ids, 'fill_counts': fill_counts, 'route_weight': route_weight}


def rms_norm(val, gain):
    v32 = val.astype(jnp.float32)
    scale = lax.rsqrt(jnp.mean(v32 * v32, axis=-1, keepdims=True) + 1e-6)
    return (v32 * scale * gain.astype(jnp.float32)).astype(jnp.bfloat16)


def rotary(vals, cos_tab, sin_tab):
    half_dim = vals.shape[-1] // 2
    v32 = vals.astype(jnp.float32)
    first = v32[..., :half_dim]
    second = v32[..., half_dim:]
    return jnp.concatenate([first * cos_tab - second * sin_tab, second * cos_tab + first * sin_tab], axis=-1).astype(jnp.bfloat16)


def attend_sequence(x_row, w_query, w_keyval, w_out, attn_gain):
    groups = HEADS // KV_HEADS
    half_dim = HEAD_DIM // 2
    normed = rms_norm(x_row, attn_gain)
    query = jnp.dot(normed, w_query.reshape(D, HEADS * HEAD_DIM), preferred_element_type=jnp.float32).astype(jnp.bfloat16).reshape(SEQ, HEADS, HEAD_DIM)
    keyval = jnp.dot(normed, w_keyval.reshape(D, 2 * KV_HEADS * HEAD_DIM), preferred_element_type=jnp.float32).astype(jnp.bfloat16).reshape(SEQ, 2 * KV_HEADS, HEAD_DIM)
    inv_freq = 10000.0 ** (-jnp.arange(half_dim, dtype=jnp.float32) / half_dim)
    angles = jnp.arange(SEQ, dtype=jnp.float32)[:, None] * inv_freq[None, :]
    cos_tab = jnp.cos(angles)[:, None, :]
    sin_tab = jnp.sin(angles)[:, None, :]
    query = rotary(query, cos_tab, sin_tab).reshape(SEQ, KV_HEADS, groups, HEAD_DIM)
    keys = rotary(keyval[:, :KV_HEADS], cos_tab, sin_tab)
    values = keyval[:, KV_HEADS:]
    scores = jnp.einsum('qhgk,shk->hgqs', query.astype(jnp.float32), keys.astype(jnp.float32)) * (HEAD_DIM ** -0.5)
    causal = jnp.arange(SEQ)[:, None] >= jnp.arange(SEQ)[None, :]
    scores = jnp.where(causal, scores, -1e30)
    attn_prob = jax.nn.softmax(scores, axis=-1).astype(jnp.bfloat16)
    mixed = jnp.einsum('hgqs,shk->qhgk', attn_prob.astype(jnp.float32), values.astype(jnp.float32)).astype(jnp.bfloat16).reshape(SEQ, HEADS * HEAD_DIM)
    attn_out = jnp.dot(mixed, w_out, preferred_element_type=jnp.float32)
    return (x_row.astype(jnp.float32) + attn_out).astype(jnp.bfloat16)


def reference(x_in, w_query, w_keyval, w_out, attn_gain, moe_gain, w_gate, w_up, w_down, expert_ids, slot_ids, fill_counts, route_weight):
    hidden = lax.map(lambda seq_row: attend_sequence(seq_row, w_query, w_keyval, w_out, attn_gain), x_in)
    h_src = hidden.reshape(GROUP, TOKENS_DEV, D)
    u_src = rms_norm(h_src, moe_gain)
    u_pad = jnp.concatenate([u_src, jnp.zeros((GROUP, 1, D), jnp.bfloat16)], axis=1)
    expert_flat = expert_ids.reshape(GROUP, TOKENS_DEV * TOP)
    slot_flat = slot_ids.reshape(GROUP, TOKENS_DEV * TOP)
    weight_flat = route_weight.reshape(GROUP, TOKENS_DEV * TOP).astype(jnp.float32)
    count_at = jnp.take_along_axis(fill_counts, expert_flat, axis=1)
    flat_pos = jnp.where(slot_flat < count_at, expert_flat * CAPACITY + slot_flat, EXPERTS * CAPACITY)
    sources = jnp.arange(GROUP)[:, None]
    tok_ids = jnp.broadcast_to(jnp.arange(TOKENS_DEV * TOP, dtype=jnp.int32) // TOP, (GROUP, TOKENS_DEV * TOP))
    slot_owner = jnp.full((GROUP, EXPERTS * CAPACITY + 1), TOKENS_DEV, jnp.int32).at[sources, flat_pos].set(tok_ids)
    slot_gate = jnp.zeros((GROUP, EXPERTS * CAPACITY + 1), jnp.float32).at[sources, flat_pos].set(weight_flat)
    slot_owner = slot_owner[:, :EXPERTS * CAPACITY].reshape(GROUP, EXPERTS, CAPACITY).transpose(1, 0, 2)
    slot_gate = slot_gate[:, :EXPERTS * CAPACITY].reshape(GROUP, EXPERTS, CAPACITY).transpose(1, 0, 2)

    def expert_step(combined, block):
        gate_mat, up_mat, down_mat, rows_owner, rows_gate = block
        in_rows = u_pad[sources, rows_owner].reshape(GROUP * CAPACITY, D)
        act_gate = jnp.dot(in_rows, gate_mat, preferred_element_type=jnp.float32)
        act_up = jnp.dot(in_rows, up_mat, preferred_element_type=jnp.float32)
        hidden_mid = (jax.nn.silu(act_gate) * act_up).astype(jnp.bfloat16)
        y_rows = jnp.dot(hidden_mid, down_mat, preferred_element_type=jnp.float32).astype(jnp.bfloat16).reshape(GROUP, CAPACITY, D)
        combined = combined.at[sources, rows_owner].add(rows_gate[..., None] * y_rows.astype(jnp.float32))
        return combined, None

    start_acc = jnp.zeros((GROUP, TOKENS_DEV + 1, D), jnp.float32)
    combined = lax.scan(expert_step, start_acc, (w_gate, w_up, w_down, slot_owner, slot_gate))[0]
    out = (h_src.astype(jnp.float32) + combined[:, :TOKENS_DEV]).astype(jnp.bfloat16)
    return out.reshape(BATCH, SEQ, D)
```

```python
import functools

import jax
import jax.numpy as jnp
from jax import lax
from jax.experimental import pallas as pl
from jax.experimental.pallas import tpu as pltpu
from jax.sharding import PartitionSpec as P

LANES = 128
QKV_ROWS = 256
ATT_ROWS = 512
OUT_ROWS = 256
MOE_ROWS = 512
CHUNKS = 4
BIG_VMEM = 60 * 1024 * 1024


def f32dot(lhs, rhs):
    return jnp.dot(lhs, rhs, preferred_element_type=jnp.float32)


def f32dot_t(lhs, rhs):
    return lax.dot_general(lhs, rhs, (((1,), (1,)), ((), ())), preferred_element_type=jnp.float32)


def rms_rows(v32, gain):
    scale = lax.rsqrt(jnp.mean(v32 * v32, axis=-1, keepdims=True) + 1e-6)
    return (v32 * scale * gain).astype(jnp.bfloat16)


def resident(shape, index_map):
    return pl.BlockSpec(shape, index_map, pipeline_mode=pl.Buffered(1))


def qkv_kernel(head_dim, q_cols, k_cols, x_ref, gain_ref, w_ref, cos_ref, sin_ref, q_ref, kk_ref, vv_ref):
    half_dim = head_dim // 2
    normed = rms_rows(x_ref[...].astype(jnp.float32), gain_ref[...].astype(jnp.float32))
    cos_tab = cos_ref[...]
    sin_tab = sin_ref[...]
    rows = x_ref.shape[0]
    lane = lax.broadcasted_iota(jnp.int32, (rows, LANES), 1)
    low_half = lax.rem(lane, head_dim) < half_dim

    def rotated(vals):
        v32 = vals.astype(jnp.bfloat16).astype(jnp.float32)
        other = jnp.where(low_half, pltpu.roll(v32, LANES - half_dim, 1), pltpu.roll(v32, half_dim, 1))
        return v32 * cos_tab + other * sin_tab

    query = f32dot(normed, w_ref[:, :q_cols])
    for c in range(q_cols // LANES):
        cols = slice(c * LANES, (c + 1) * LANES)
        q_ref[:, cols] = rotated(query[:, cols]).astype(jnp.bfloat16)
    keys = f32dot(normed, w_ref[:, q_cols:q_cols + k_cols])
    for c in range(k_cols // LANES):
        cols = slice(c * LANES, (c + 1) * LANES)
        rot = rotated(keys[:, cols]).astype(jnp.bfloat16).astype(jnp.float32)
        kk_ref[0, :, cols] = rot.astype(jnp.bfloat16)
        kk_ref[1, :, cols] = pltpu.roll(rot, head_dim, 1).astype(jnp.bfloat16)
    values = f32dot(normed, w_ref[:, q_cols + k_cols:])
    for c in range(k_cols // LANES):
        cols = slice(c * LANES, (c + 1) * LANES)
        val = values[:, cols].astype(jnp.bfloat16).astype(jnp.float32)
        vv_ref[0, :, cols] = val.astype(jnp.bfloat16)
        vv_ref[1, :, cols] = pltpu.roll(val, head_dim, 1).astype(jnp.bfloat16)


def qkv_call(x_rows, gain, w_qkv, cos_tab, sin_tab, head_dim, q_cols, k_cols):
    tokens, width = x_rows.shape
    rows = QKV_ROWS
    return pl.pallas_call(
        functools.partial(qkv_kernel, head_dim, q_cols, k_cols),
        grid=(tokens // rows,),
        in_specs=[
            pl.BlockSpec((rows, width), lambda i: (i, 0)),
            resident((1, width), lambda i: (0, 0)),
            resident(w_qkv.shape, lambda i: (0, 0)),
            pl.BlockSpec((rows, LANES), lambda i: (i, 0)),
            pl.BlockSpec((rows, LANES), lambda i: (i, 0)),
        ],
        out_specs=[
            pl.BlockSpec((rows, q_cols), lambda i: (i, 0)),
            pl.BlockSpec((2, rows, k_cols), lambda i: (0, i, 0)),
            pl.BlockSpec((2, rows, k_cols), lambda i: (0, i, 0)),
        ],
        out_shape=[
            jax.ShapeDtypeStruct((tokens, q_cols), jnp.bfloat16),
            jax.ShapeDtypeStruct((2, tokens, k_cols), jnp.bfloat16),
            jax.ShapeDtypeStruct((2, tokens, k_cols), jnp.bfloat16),
        ],
        compiler_params=pltpu.CompilerParams(vmem_limit_bytes=BIG_VMEM),
        cost_estimate=pl.CostEstimate(flops=2 * tokens * width * w_qkv.shape[1], bytes_accessed=tokens * width * 10, transcendentals=0),
        name='qkv_rope',
    )(x_rows, gain, w_qkv, cos_tab, sin_tab)


def attend_kernel(head_dim, q_ref, ka_ref, kb_ref, va_ref, vb_ref, o_ref, s_buf, m_buf, l_buf, o_buf):
    rows = q_ref.shape[0]
    step = pl.program_id(1)
    lane = lax.broadcasted_iota(jnp.int32, (rows, LANES), 1)
    low = lane < head_dim
    query = q_ref[...].astype(jnp.float32) * (head_dim ** -0.5)
    zero = jnp.zeros_like(query)
    heads = (jnp.where(low, query, zero).astype(jnp.bfloat16), jnp.where(low, zero, query).astype(jnp.bfloat16))
    key_refs = (ka_ref, kb_ref)
    val_refs = (va_ref, vb_ref)
    groups = rows // LANES

    def span(blk):
        return pl.ds(pl.multiple_of(blk * rows, rows), rows)

    def fold(op, tile):
        out = tile[:, :LANES]
        for g in range(1, groups):
            out = op(out, tile[:, g * LANES:(g + 1) * LANES])
        return out

    def scores(head, blk, masked):
        tile = f32dot_t(heads[head], key_refs[head][0, span(blk), :])
        if masked:
            row_id = lax.broadcasted_iota(jnp.int32, (rows, rows), 0)
            col_id = lax.broadcasted_iota(jnp.int32, (rows, rows), 1)
            tile = jnp.where(row_id >= col_id, tile, -1e30)
        s_buf[head, :, span(blk)] = tile
        m_buf[head] = jnp.maximum(m_buf[head], fold(jnp.maximum, tile))

    def exps(head, blk, row_max):
        tile = jnp.exp(s_buf[head, :, span(blk)] - row_max)
        s_buf[head, :, span(blk)] = tile
        l_buf[head] += fold(jnp.add, tile)

    def mixes(head, blk, inv_sum):
        prob = (s_buf[head, :, span(blk)] * inv_sum).astype(jnp.bfloat16)
        o_buf[head] += f32dot(prob, val_refs[head][0, span(blk), :])

    m_buf[...] = jnp.full_like(m_buf, -1e30)
    l_buf[...] = jnp.zeros_like(l_buf)
    o_buf[...] = jnp.zeros_like(o_buf)

    @pl.loop(0, step)
    def _(blk):
        scores(0, blk, False)

    scores(0, step, True)
    max0 = jnp.max(m_buf[0], axis=-1, keepdims=True)

    @pl.loop(0, step)
    def _(blk):
        scores(1, blk, False)
        exps(0, blk, max0)

    scores(1, step, True)
    exps(0, step, max0)
    max1 = jnp.max(m_buf[1], axis=-1, keepdims=True)
    inv0 = 1.0 / jnp.sum(l_buf[0], axis=-1, keepdims=True)

    @pl.loop(0, step + 1)
    def _(blk):
        mixes(0, blk, inv0)
        exps(1, blk, max1)

    inv1 = 1.0 / jnp.sum(l_buf[1], axis=-1, keepdims=True)

    @pl.loop(0, step + 1)
    def _(blk):
        mixes(1, blk, inv1)

    o_ref[...] = jnp.where(low, o_buf[0], o_buf[1]).astype(jnp.bfloat16)


def attend_call(query, keys, values, head_dim):
    tokens, q_cols = query.shape
    kv_heads = keys.shape[2] // head_dim
    rows = min(ATT_ROWS, tokens)
    per_tile = LANES // head_dim
    kv_block = (1, tokens, LANES)
    same = lambda h, i: (h % per_tile, 0, h // per_tile)
    other = lambda h, i: (1 - h % per_tile, 0, h // per_tile)
    return pl.pallas_call(
        functools.partial(attend_kernel, head_dim),
        grid=(kv_heads, tokens // rows),
        in_specs=[
            pl.BlockSpec((rows, LANES), lambda h, i: (i, h)),
            pl.BlockSpec(kv_block, same),
            pl.BlockSpec(kv_block, other),
            pl.BlockSpec(kv_block, same),
            pl.BlockSpec(kv_block, other),
        ],
        out_specs=pl.BlockSpec((rows, LANES), lambda h, i: (i, h)),
        out_shape=jax.ShapeDtypeStruct((tokens, q_cols), jnp.bfloat16),
        scratch_shapes=[
            pltpu.VMEM((2, rows, tokens), jnp.float32),
            pltpu.VMEM((2, rows, LANES), jnp.float32),
            pltpu.VMEM((2, rows, LANES), jnp.float32),
            pltpu.VMEM((2, rows, LANES), jnp.float32),
        ],
        compiler_params=pltpu.CompilerParams(vmem_limit_bytes=BIG_VMEM),
        cost_estimate=pl.CostEstimate(flops=8 * tokens * tokens * q_cols, bytes_accessed=tokens * q_cols * 12, transcendentals=tokens * tokens * q_cols // LANES),
        name='attend',
    )(query, keys, keys, values, values)


def out_kernel(mixed_ref, w_ref, x_ref, gain_ref, h_ref, u_ref):
    hidden = (x_ref[...].astype(jnp.float32) + f32dot(mixed_ref[...], w_ref[...])).astype(jnp.bfloat16)
    h_ref[...] = hidden
    u_ref[...] = rms_rows(hidden.astype(jnp.float32), gain_ref[...].astype(jnp.float32))


def out_call(mixed, w_out, x_rows, gain):
    tokens, width = x_rows.shape
    rows = OUT_ROWS
    block = pl.BlockSpec((rows, width), lambda i: (i, 0))
    return pl.pallas_call(
        out_kernel,
        grid=(tokens // rows,),
        in_specs=[
            pl.BlockSpec((rows, mixed.shape[1]), lambda i: (i, 0)),
            resident(w_out.shape, lambda i: (0, 0)),
            block,
            resident((1, width), lambda i: (0, 0)),
        ],
        out_specs=[block, block],
        out_shape=[jax.ShapeDtypeStruct((tokens, width), jnp.bfloat16)] * 2,
        compiler_params=pltpu.CompilerParams(vmem_limit_bytes=BIG_VMEM),
        cost_estimate=pl.CostEstimate(flops=2 * tokens * width * mixed.shape[1], bytes_accessed=tokens * width * 10, transcendentals=0),
        name='out_proj',
    )(mixed, w_out, x_rows, gain)


def moe_kernel(first_expert, is_first, is_last, u_ref, gate_ref, w_ref, *rest):
    if is_first:
        rest = (None,) + rest
    acc_in, *rest = rest
    if is_last:
        h_ref, out_ref, acc, sem = rest
    else:
        out_ref, acc, sem = rest
    step = pl.program_id(0)
    expert = first_expert + step
    shards, _, _, depth, inner = w_ref.shape
    full = shards * depth

    @pl.when(step == 0)
    def _():
        if is_first:
            acc[...] = jnp.zeros_like(acc)
        else:
            copy = pltpu.make_async_copy(acc_in, acc, sem)
            copy.start()
            copy.wait()

    w_gate = w_ref[:, 0, 0].reshape(full, inner)
    w_up = w_ref[:, 1, 0].reshape(full, inner)
    w_down = w_ref[:, 2, 0].reshape(full, inner)
    tokens = u_ref.shape[0]

    @pl.loop(0, tokens // MOE_ROWS)
    def _(blk):
        rows = pl.ds(pl.multiple_of(blk * MOE_ROWS, MOE_ROWS), MOE_ROWS)
        in_rows = u_ref[rows, :]
        hidden_mid = (jax.nn.silu(f32dot(in_rows, w_gate)) * f32dot(in_rows, w_up)).astype(jnp.bfloat16)
        y_rows = f32dot_t(hidden_mid, w_down).astype(jnp.bfloat16).astype(jnp.float32)
        gates = gate_ref[rows, :]
        lane = lax.broadcasted_iota(jnp.int32, gates.shape, 1)
        weight = jnp.sum(jnp.where(lane == expert, gates, 0.0), axis=-1, keepdims=True)
        acc[rows, :] += jnp.where(weight > 0, weight * y_rows, 0.0)

    @pl.when(step == pl.num_programs(0) - 1)
    def _():
        if is_last:
            @pl.loop(0, tokens // MOE_ROWS)
            def _(blk):
                rows = pl.ds(pl.multiple_of(blk * MOE_ROWS, MOE_ROWS), MOE_ROWS)
                out_ref[rows, :] = (h_ref[rows, :].astype(jnp.float32) + acc[rows, :]).astype(jnp.bfloat16)
        else:
            copy = pltpu.make_async_copy(acc, out_ref, sem)
            copy.start()
            copy.wait()


def moe_call(u_rows, gates, weights, acc, h_rows, first_expert, is_last):
    tokens, width = u_rows.shape
    shards, parts, count, depth, inner = weights.shape
    is_first = acc is None
    whole = lambda e: (0, 0)
    args = [u_rows, gates, weights]
    in_specs = [
        resident((tokens, width), whole),
        resident(gates.shape, whole),
        pl.BlockSpec((shards, parts, 1, depth, inner), lambda e: (0, 0, e, 0, 0)),
    ]
    aliases = {}
    if not is_first:
        args.append(acc)
        in_specs.append(pl.BlockSpec(memory_space=pl.ANY))
        if not is_last:
            aliases = {3: 0}
    if is_last:
        args.append(h_rows)
        in_specs.append(resident((tokens, width), whole))
        out_spec = resident((tokens, width), whole)
        out_shape = jax.ShapeDtypeStruct((tokens, width), jnp.bfloat16)
    else:
        out_spec = pl.BlockSpec(memory_space=pl.ANY)
        out_shape = jax.ShapeDtypeStruct((tokens, width), jnp.float32)
    return pl.pallas_call(
        functools.partial(moe_kernel, first_expert, is_first, is_last),
        grid=(count,),
        in_specs=in_specs,
        out_specs=out_spec,
        out_shape=out_shape,
        scratch_shapes=[pltpu.VMEM((tokens, width), jnp.float32), pltpu.SemaphoreType.DMA],
        input_output_aliases=aliases,
        compiler_params=pltpu.CompilerParams(vmem_limit_bytes=BIG_VMEM),
        cost_estimate=pl.CostEstimate(flops=6 * tokens * width * inner * count, bytes_accessed=2 * weights.size + 16 * tokens * width, transcendentals=tokens * inner * count),
        name='moe_part',
    )(*args)


def gate_table(expert_ids, slot_ids, counts, weights):
    tokens, choices = expert_ids.shape
    limits = jnp.pad(counts, (0, LANES - counts.shape[0]))[None, :]
    lane = lax.broadcasted_iota(jnp.int32, (tokens, LANES), 1)
    table = jnp.zeros((tokens, LANES), jnp.float32)
    for k in range(choices):
        kept = (expert_ids[:, k:k + 1] == lane) & (slot_ids[:, k:k + 1] < limits)
        table = jnp.where(kept, weights[:, k:k + 1].astype(jnp.float32), table)
    return table


def local_layer(x_rows, w_qkv, w_out, attn_gain, moe_gain, expert_parts, gates, head_dim, q_cols, k_cols):
    tokens, width = x_rows.shape
    half_dim = head_dim // 2
    inv_freq = 10000.0 ** (-jnp.arange(half_dim, dtype=jnp.float32) / half_dim)
    angles = jnp.arange(tokens, dtype=jnp.float32)[:, None] * inv_freq[None, :]
    cos_half, sin_half = jnp.cos(angles), jnp.sin(angles)
    reps = LANES // head_dim
    cos_tab = jnp.tile(cos_half, (1, 2 * reps))
    sin_tab = jnp.tile(jnp.concatenate([-sin_half, sin_half], axis=1), (1, reps))
    query, keys, values = qkv_call(x_rows, attn_gain[None, :], w_qkv, cos_tab, sin_tab, head_dim, q_cols, k_cols)
    mixed = attend_call(query, keys, values, head_dim)
    h_rows, u_rows = out_call(mixed, w_out, x_rows, moe_gain[None, :])
    acc = None
    first = 0
    for i, part in enumerate(expert_parts):
        acc = moe_call(u_rows, gates, part, acc, h_rows, first, i == len(expert_parts) - 1)
        first += part.shape[2]
    return acc


def solution(mesh):
    row_spec = P(('data', 'ep'))

    def device_step(x_in, w_query, w_keyval, w_out, attn_gain, moe_gain, w_gate, w_up, w_down, expert_ids, slot_ids, fill_counts, route_weight):
        batch_loc, seq_len, model_dim = x_in.shape
        rows_loc, num_heads, head_dim = w_query.shape
        q_cols = num_heads * head_dim
        k_cols = w_keyval.shape[1] // 2 * head_dim
        experts = w_gate.shape[0]
        choices = expert_ids.shape[-1]
        w_local = jnp.concatenate([w_query.reshape(rows_loc, q_cols), w_keyval.reshape(rows_loc, 2 * k_cols)], axis=1)
        w_qkv = lax.all_gather(w_local, 'ep', axis=0, tiled=True)
        per = experts // CHUNKS
        mats = (w_gate, w_up, jnp.swapaxes(w_down, 1, 2))
        stacks = [jnp.stack([mat[c * per:(c + 1) * per] for mat in mats]) for c in range(CHUNKS)]
        stacks, w_out, w_qkv = lax.optimization_barrier((stacks, w_out, w_qkv))
        full_out = lax.all_gather(w_out, 'ep', axis=0, tiled=True)
        expert_parts = [lax.all_gather(part, 'ep', axis=0, tiled=False) for part in stacks]
        outs = []
        for b in range(batch_loc):
            gates = gate_table(expert_ids[b], slot_ids[b], fill_counts[0], route_weight[b])
            outs.append(local_layer(x_in[b], w_qkv, full_out, attn_gain, moe_gain, expert_parts, gates, head_dim, q_cols, k_cols))
        return jnp.stack(outs)

    in_specs = (row_spec, P('ep'), P('ep'), P('ep'), P(), P(), P(None, 'ep'), P(None, 'ep'), P(None, None, 'ep'), row_spec, row_spec, row_spec, row_spec)
    return jax.shard_map(device_step, mesh=mesh, in_specs=in_specs, out_specs=row_spec, check_vma=False)
```

```python
import functools

import jax
import jax.numpy as jnp
from jax import lax
from jax.experimental import pallas as pl
from jax.experimental.pallas import tpu as pltpu
from jax.sharding import PartitionSpec as P

LANES = 128
QKV_ROWS = 256
ATT_ROWS = 512
OUT_ROWS = 256
MOE_ROWS = 512
MOE_PAIR = 2
SHARES = (14, 11, 7)
BIG_VMEM = 60 * 1024 * 1024


def f32dot(lhs, rhs):
    return jnp.dot(lhs, rhs, preferred_element_type=jnp.float32)


def f32dot_t(lhs, rhs):
    return lax.dot_general(lhs, rhs, (((1,), (1,)), ((), ())), preferred_element_type=jnp.float32)


def rms_rows(v32, gain):
    scale = lax.rsqrt(jnp.mean(v32 * v32, axis=-1, keepdims=True) + 1e-6)
    return (v32 * scale * gain).astype(jnp.bfloat16)


def resident(shape, index_map):
    return pl.BlockSpec(shape, index_map, pipeline_mode=pl.Buffered(1))


def qkv_kernel(head_dim, q_cols, k_cols, x_ref, gain_ref, w_ref, cos_ref, sin_ref, q_ref, kk_ref, vv_ref):
    half_dim = head_dim // 2
    normed = rms_rows(x_ref[...].astype(jnp.float32), gain_ref[...].astype(jnp.float32))
    cos_tab = cos_ref[...]
    sin_tab = sin_ref[...]
    rows = x_ref.shape[0]
    lane = lax.broadcasted_iota(jnp.int32, (rows, LANES), 1)
    low_half = lax.rem(lane, head_dim) < half_dim

    def rotated(vals):
        v32 = vals.astype(jnp.bfloat16).astype(jnp.float32)
        other = jnp.where(low_half, pltpu.roll(v32, LANES - half_dim, 1), pltpu.roll(v32, half_dim, 1))
        return v32 * cos_tab + other * sin_tab

    query = f32dot(normed, w_ref[:, :q_cols])
    for c in range(q_cols // LANES):
        cols = slice(c * LANES, (c + 1) * LANES)
        q_ref[:, cols] = rotated(query[:, cols]).astype(jnp.bfloat16)
    keys = f32dot(normed, w_ref[:, q_cols:q_cols + k_cols])
    for c in range(k_cols // LANES):
        cols = slice(c * LANES, (c + 1) * LANES)
        rot = rotated(keys[:, cols]).astype(jnp.bfloat16).astype(jnp.float32)
        kk_ref[0, :, cols] = rot.astype(jnp.bfloat16)
        kk_ref[1, :, cols] = pltpu.roll(rot, head_dim, 1).astype(jnp.bfloat16)
    values = f32dot(normed, w_ref[:, q_cols + k_cols:])
    for c in range(k_cols // LANES):
        cols = slice(c * LANES, (c + 1) * LANES)
        val = values[:, cols].astype(jnp.bfloat16).astype(jnp.float32)
        vv_ref[0, :, cols] = val.astype(jnp.bfloat16)
        vv_ref[1, :, cols] = pltpu.roll(val, head_dim, 1).astype(jnp.bfloat16)


def qkv_call(x_rows, gain, w_qkv, cos_tab, sin_tab, head_dim, q_cols, k_cols):
    tokens, width = x_rows.shape
    rows = QKV_ROWS
    return pl.pallas_call(
        functools.partial(qkv_kernel, head_dim, q_cols, k_cols),
        grid=(tokens // rows,),
        in_specs=[
            pl.BlockSpec((rows, width), lambda i: (i, 0)),
            resident((1, width), lambda i: (0, 0)),
            resident((width, q_cols + 2 * k_cols), lambda i: (0, 0)),
            pl.BlockSpec((rows, LANES), lambda i: (i, 0)),
            pl.BlockSpec((rows, LANES), lambda i: (i, 0)),
        ],
        out_specs=[
            pl.BlockSpec((rows, q_cols), lambda i: (i, 0)),
            pl.BlockSpec((2, rows, k_cols), lambda i: (0, i, 0)),
            pl.BlockSpec((2, rows, k_cols), lambda i: (0, i, 0)),
        ],
        out_shape=[
            jax.ShapeDtypeStruct((tokens, q_cols), jnp.bfloat16),
            jax.ShapeDtypeStruct((2, tokens, k_cols), jnp.bfloat16),
            jax.ShapeDtypeStruct((2, tokens, k_cols), jnp.bfloat16),
        ],
        compiler_params=pltpu.CompilerParams(vmem_limit_bytes=BIG_VMEM),
        cost_estimate=pl.CostEstimate(flops=2 * tokens * width * (q_cols + 2 * k_cols), bytes_accessed=tokens * width * 10, transcendentals=0),
        name='qkv_rope',
    )(x_rows, gain, w_qkv, cos_tab, sin_tab)


def attend_kernel(head_dim, q_ref, ka_ref, kb_ref, va_ref, vb_ref, o_ref, q_buf, s_buf):
    rows = q_ref.shape[0]
    half = rows // 2
    tokens = ka_ref.shape[1]
    step = pl.program_id(1)
    lane = lax.broadcasted_iota(jnp.int32, (rows, LANES), 1)
    low = lane < head_dim
    query = q_ref[...].astype(jnp.float32) * (head_dim ** -0.5)
    zero = jnp.zeros_like(query)
    q_buf[0] = jnp.where(low, query, zero).astype(jnp.bfloat16)
    q_buf[1] = jnp.where(low, zero, query).astype(jnp.bfloat16)
    key_refs = (ka_ref, kb_ref)
    val_refs = (va_ref, vb_ref)

    def fold(op, tile, out):
        for g in range(tile.shape[1] // LANES):
            part = tile[:, g * LANES:(g + 1) * LANES]
            out = part if out is None else op(out, part)
        return out

    def run_case(case):
        chains = [dict(head=head, part=part, top=None, total=None, out=None) for part in range(2) for head in range(2)]
        for chain in chains:
            diag = (2 * case + chain['part']) * half
            pieces = []
            start = 0
            while start < diag:
                width = min(rows, diag - start)
                pieces.append((start, width, False))
                start += width
            chain['pieces'] = pieces + [(diag, half, True)]

        def scores(slot, chain, piece):
            start, width, masked = piece
            own = q_buf[chain['head'], chain['part'] * half:(chain['part'] + 1) * half, :]
            tile = f32dot_t(own, key_refs[chain['head']][0, start:start + width, :])
            if masked:
                row_id = lax.broadcasted_iota(jnp.int32, (half, width), 0)
                col_id = lax.broadcasted_iota(jnp.int32, (half, width), 1)
                tile = jnp.where(row_id >= col_id, tile, -1e30)
            s_buf[slot, :, start:start + width] = tile
            chain['top'] = fold(jnp.maximum, tile, chain['top'])

        def exps(slot, chain, piece):
            start, width, _ = piece
            tile = jnp.exp(s_buf[slot, :, start:start + width] - chain['row_max'])
            s_buf[slot, :, start:start + width] = tile
            chain['total'] = fold(jnp.add, tile, chain['total'])

        def mixes(slot, chain, piece):
            start, width, _ = piece
            prob = (s_buf[slot, :, start:start + width] * chain['inv']).astype(jnp.bfloat16)
            part = f32dot(prob, val_refs[chain['head']][0, start:start + width, :])
            chain['out'] = part if chain['out'] is None else chain['out'] + part

        count = len(chains)
        for slot in range(count + 2):
            work = []
            if slot < count:
                work.append((scores, slot))
            if 0 <= slot - 1 < count:
                chain = chains[slot - 1]
                chain['row_max'] = jnp.max(chain['top'], axis=-1, keepdims=True)
                work.append((exps, slot - 1))
            if 0 <= slot - 2 < count:
                chain = chains[slot - 2]
                chain['inv'] = 1.0 / jnp.sum(chain['total'], axis=-1, keepdims=True)
                work.append((mixes, slot - 2))
            for j in range(max(len(chains[i]['pieces']) for _, i in work)):
                for stage, i in work:
                    if j < len(chains[i]['pieces']):
                        stage(i, chains[i], chains[i]['pieces'][j])
        low_half = low[:half]
        for part in range(2):
            first, second = chains[2 * part]['out'], chains[2 * part + 1]['out']
            o_ref[part * half:(part + 1) * half, :] = jnp.where(low_half, first, second).astype(jnp.bfloat16)

    for case in range(tokens // rows):
        pl.when(step == case)(functools.partial(run_case, case))


def attend_call(query, keys, values, head_dim):
    tokens, q_cols = query.shape
    kv_heads = keys.shape[2] // head_dim
    rows = min(ATT_ROWS, tokens)
    per_tile = LANES // head_dim
    kv_block = (1, tokens, LANES)
    same = lambda h, i: (h % per_tile, 0, h // per_tile)
    other = lambda h, i: (1 - h % per_tile, 0, h // per_tile)
    return pl.pallas_call(
        functools.partial(attend_kernel, head_dim),
        grid=(kv_heads, tokens // rows),
        in_specs=[
            pl.BlockSpec((rows, LANES), lambda h, i: (i, h)),
            pl.BlockSpec(kv_block, same),
            pl.BlockSpec(kv_block, other),
            pl.BlockSpec(kv_block, same),
            pl.BlockSpec(kv_block, other),
        ],
        out_specs=pl.BlockSpec((rows, LANES), lambda h, i: (i, h)),
        out_shape=jax.ShapeDtypeStruct((tokens, q_cols), jnp.bfloat16),
        scratch_shapes=[
            pltpu.VMEM((2, rows, LANES), jnp.bfloat16),
            pltpu.VMEM((4, rows // 2, tokens), jnp.float32),
        ],
        compiler_params=pltpu.CompilerParams(vmem_limit_bytes=BIG_VMEM),
        cost_estimate=pl.CostEstimate(flops=8 * tokens * tokens * q_cols, bytes_accessed=tokens * q_cols * 12, transcendentals=tokens * tokens * q_cols // LANES),
        name='attend',
    )(query, keys, keys, values, values)


def out_kernel(mixed_ref, w_ref, x_ref, gain_ref, h_ref, u_ref):
    hidden = (x_ref[...].astype(jnp.float32) + f32dot(mixed_ref[...], w_ref[...])).astype(jnp.bfloat16)
    h_ref[...] = hidden
    u_ref[...] = rms_rows(hidden.astype(jnp.float32), gain_ref[...].astype(jnp.float32))


def out_call(mixed, w_attn, x_rows, gain):
    tokens, width = x_rows.shape
    rows = OUT_ROWS
    block = pl.BlockSpec((rows, width), lambda i: (i, 0))
    return pl.pallas_call(
        out_kernel,
        grid=(tokens // rows,),
        in_specs=[
            pl.BlockSpec((rows, mixed.shape[1]), lambda i: (i, 0)),
            resident((mixed.shape[1], width), lambda i: (0, w_attn.shape[1] // width - 1)),
            block,
            resident((1, width), lambda i: (0, 0)),
        ],
        out_specs=[block, block],
        out_shape=[jax.ShapeDtypeStruct((tokens, width), jnp.bfloat16)] * 2,
        compiler_params=pltpu.CompilerParams(vmem_limit_bytes=BIG_VMEM),
        cost_estimate=pl.CostEstimate(flops=2 * tokens * width * mixed.shape[1], bytes_accessed=tokens * width * 10, transcendentals=0),
        name='out_proj',
    )(mixed, w_attn, x_rows, gain)


def moe_kernel(first_expert, is_first, is_last, u_ref, gate_ref, w_ref, *rest):
    if is_first:
        rest = (None,) + rest
    acc_in, *rest = rest
    if is_last:
        h_ref, out_ref, acc, sem = rest
    else:
        out_ref, acc, sem = rest
    step = pl.program_id(0)
    expert = first_expert + step
    shards, _, _, depth, inner = w_ref.shape
    full = shards * depth

    @pl.when(step == 0)
    def _():
        if is_first:
            acc[...] = jnp.zeros_like(acc)
        else:
            copy = pltpu.make_async_copy(acc_in, acc, sem)
            copy.start()
            copy.wait()

    tokens = u_ref.shape[0]

    @pl.loop(0, tokens // (MOE_PAIR * MOE_ROWS))
    def _(trip):
        def span(i):
            return pl.ds(pl.multiple_of((trip * MOE_PAIR + i) * MOE_ROWS, MOE_ROWS), MOE_ROWS)

        def matrix(i):
            return w_ref[:, i, 0].reshape(full, inner)

        mids = []
        for i in range(MOE_PAIR):
            in_rows = u_ref[span(i), :]
            mids.append((jax.nn.silu(f32dot(in_rows, matrix(0))) * f32dot(in_rows, matrix(1))).astype(jnp.bfloat16))
        for i in range(MOE_PAIR):
            y_rows = f32dot_t(mids[i], matrix(2)).astype(jnp.bfloat16).astype(jnp.float32)
            gates = gate_ref[span(i), :]
            lane = lax.broadcasted_iota(jnp.int32, gates.shape, 1)
            weight = jnp.sum(jnp.where(lane == expert, gates, 0.0), axis=-1, keepdims=True)
            acc[span(i), :] += jnp.where(weight > 0, weight * y_rows, 0.0)

    @pl.when(step == pl.num_programs(0) - 1)
    def _():
        if is_last:
            @pl.loop(0, tokens // MOE_ROWS)
            def _(blk):
                rows = pl.ds(pl.multiple_of(blk * MOE_ROWS, MOE_ROWS), MOE_ROWS)
                out_ref[rows, :] = (h_ref[rows, :].astype(jnp.float32) + acc[rows, :]).astype(jnp.bfloat16)
        else:
            copy = pltpu.make_async_copy(acc, out_ref, sem)
            copy.start()
            copy.wait()


def moe_call(u_rows, gates, weights, acc, h_rows, first_expert, is_last):
    tokens, width = u_rows.shape
    shards, parts, count, depth, inner = weights.shape
    is_first = acc is None
    whole = lambda e: (0, 0)
    args = [u_rows, gates, weights]
    in_specs = [
        resident((tokens, width), whole),
        resident(gates.shape, whole),
        pl.BlockSpec((shards, parts, 1, depth, inner), lambda e: (0, 0, e, 0, 0)),
    ]
    aliases = {}
    if not is_first:
        args.append(acc)
        in_specs.append(pl.BlockSpec(memory_space=pl.ANY))
        if not is_last:
            aliases = {3: 0}
    if is_last:
        args.append(h_rows)
        in_specs.append(resident((tokens, width), whole))
        out_spec = resident((tokens, width), whole)
        out_shape = jax.ShapeDtypeStruct((tokens, width), jnp.bfloat16)
    else:
        out_spec = pl.BlockSpec(memory_space=pl.ANY)
        out_shape = jax.ShapeDtypeStruct((tokens, width), jnp.float32)
    return pl.pallas_call(
        functools.partial(moe_kernel, first_expert, is_first, is_last),
        grid=(count,),
        in_specs=in_specs,
        out_specs=out_spec,
        out_shape=out_shape,
        scratch_shapes=[pltpu.VMEM((tokens, width), jnp.float32), pltpu.SemaphoreType.DMA],
        input_output_aliases=aliases,
        compiler_params=pltpu.CompilerParams(vmem_limit_bytes=BIG_VMEM),
        cost_estimate=pl.CostEstimate(flops=6 * tokens * width * inner * count, bytes_accessed=2 * weights.size + 16 * tokens * width, transcendentals=tokens * inner * count),
        name='moe_part',
    )(*args)


def gate_table(expert_ids, slot_ids, counts, weights):
    tokens, choices = expert_ids.shape
    limits = jnp.pad(counts, (0, LANES - counts.shape[0]))[None, :]
    lane = lax.broadcasted_iota(jnp.int32, (tokens, LANES), 1)
    table = jnp.zeros((tokens, LANES), jnp.float32)
    for k in range(choices):
        kept = (expert_ids[:, k:k + 1] == lane) & (slot_ids[:, k:k + 1] < limits)
        table = jnp.where(kept, weights[:, k:k + 1].astype(jnp.float32), table)
    return table


def rotary_tables(tokens, head_dim):
    half_dim = head_dim // 2
    inv_freq = 10000.0 ** (-jnp.arange(half_dim, dtype=jnp.float32) / half_dim)
    angles = jnp.arange(tokens, dtype=jnp.float32)[:, None] * inv_freq[None, :]
    cos_half, sin_half = jnp.cos(angles), jnp.sin(angles)
    reps = LANES // head_dim
    return jnp.tile(cos_half, (1, 2 * reps)), jnp.tile(jnp.concatenate([-sin_half, sin_half], axis=1), (1, reps))


def local_layer(x_rows, w_attn, attn_gain, moe_gain, expert_parts, gates, tables, head_dim, q_cols, k_cols):
    query, keys, values = qkv_call(x_rows, attn_gain, w_attn, *tables, head_dim, q_cols, k_cols)
    mixed = attend_call(query, keys, values, head_dim)
    h_rows, u_rows = out_call(mixed, w_attn, x_rows, moe_gain)
    acc = None
    first = 0
    for i, part in enumerate(expert_parts):
        acc = moe_call(u_rows, gates, part, acc, h_rows, first, i == len(expert_parts) - 1)
        first += part.shape[2]
    return acc


def shares_of(experts):
    total = sum(SHARES)
    sizes = [experts * share // total for share in SHARES[1:]]
    return [experts - sum(sizes)] + sizes


def solution(mesh):
    row_spec = P(('data', 'ep'))

    def device_step(x_in, w_query, w_keyval, w_out, attn_gain, moe_gain, w_gate, w_up, w_down, expert_ids, slot_ids, fill_counts, route_weight):
        batch_loc, seq_len, model_dim = x_in.shape
        rows_loc, num_heads, head_dim = w_query.shape
        q_cols = num_heads * head_dim
        k_cols = w_keyval.shape[1] // 2 * head_dim
        experts = w_gate.shape[0]
        w_local = jnp.concatenate([w_query.reshape(rows_loc, q_cols), w_keyval.reshape(rows_loc, 2 * k_cols), w_out], axis=1)
        w_attn = lax.all_gather(w_local, 'ep', axis=0, tiled=True)
        mats = (w_gate, w_up, jnp.swapaxes(w_down, 1, 2))
        stacks = []
        first = 0
        for size in shares_of(experts):
            stacks.append(jnp.stack([mat[first:first + size] for mat in mats]))
            first += size
        tables = rotary_tables(seq_len, head_dim)
        gates = [gate_table(expert_ids[b], slot_ids[b], fill_counts[0], route_weight[b]) for b in range(batch_loc)]
        gains = (attn_gain[None, :], moe_gain[None, :])
        stacks, tables, gates, gains, w_attn = lax.optimization_barrier((stacks, tables, gates, gains, w_attn))
        expert_parts = [lax.all_gather(part, 'ep', axis=0, tiled=False) for part in stacks]
        outs = []
        for b in range(batch_loc):
            outs.append(local_layer(x_in[b], w_attn, *gains, expert_parts, gates[b], tables, head_dim, q_cols, k_cols))
        return jnp.stack(outs)

    in_specs = (row_spec, P('ep'), P('ep'), P('ep'), P(), P(), P(None, 'ep'), P(None, 'ep'), P(None, None, 'ep'), row_spec, row_spec, row_spec, row_spec)
    return jax.shard_map(device_step, mesh=mesh, in_specs=in_specs, out_specs=row_spec, check_vma=False)
```

```python
import functools

import jax
import jax.numpy as jnp
from jax import lax
from jax.experimental import pallas as pl
from jax.experimental.pallas import tpu as pltpu
from jax.sharding import PartitionSpec as P

LANES = 128
QKV_ROWS = 256
ATT_ROWS = 512
OUT_ROWS = 256
MOE_ROWS = 512
MOE_PAIR = 2
FEW_ROWS = 256
SHARES = (16, 10, 6)
BIG_VMEM = 60 * 1024 * 1024


def f32dot(lhs, rhs):
    return jnp.dot(lhs, rhs, preferred_element_type=jnp.float32)


def f32dot_t(lhs, rhs):
    return lax.dot_general(lhs, rhs, (((1,), (1,)), ((), ())), preferred_element_type=jnp.float32)


def rms_rows(v32, gain):
    scale = lax.rsqrt(jnp.mean(v32 * v32, axis=-1, keepdims=True) + 1e-6)
    return (v32 * scale * gain).astype(jnp.bfloat16)


def resident(shape, index_map):
    return pl.BlockSpec(shape, index_map, pipeline_mode=pl.Buffered(1))


def qkv_kernel(head_dim, q_cols, k_cols, x_ref, gain_ref, w_ref, cos_ref, sin_ref, q_ref, kk_ref, vv_ref):
    half_dim = head_dim // 2
    normed = rms_rows(x_ref[...].astype(jnp.float32), gain_ref[...].astype(jnp.float32))
    cos_tab = cos_ref[...]
    sin_tab = sin_ref[...]
    rows = x_ref.shape[0]
    lane = lax.broadcasted_iota(jnp.int32, (rows, LANES), 1)
    low_half = lax.rem(lane, head_dim) < half_dim

    def rotated(vals):
        v32 = vals.astype(jnp.bfloat16).astype(jnp.float32)
        other = jnp.where(low_half, pltpu.roll(v32, LANES - half_dim, 1), pltpu.roll(v32, half_dim, 1))
        return v32 * cos_tab + other * sin_tab

    query = f32dot(normed, w_ref[:, :q_cols])
    for c in range(q_cols // LANES):
        cols = slice(c * LANES, (c + 1) * LANES)
        q_ref[:, cols] = rotated(query[:, cols]).astype(jnp.bfloat16)
    keys = f32dot(normed, w_ref[:, q_cols:q_cols + k_cols])
    for c in range(k_cols // LANES):
        cols = slice(c * LANES, (c + 1) * LANES)
        rot = rotated(keys[:, cols]).astype(jnp.bfloat16).astype(jnp.float32)
        kk_ref[0, :, cols] = rot.astype(jnp.bfloat16)
        kk_ref[1, :, cols] = pltpu.roll(rot, head_dim, 1).astype(jnp.bfloat16)
    values = f32dot(normed, w_ref[:, q_cols + k_cols:])
    for c in range(k_cols // LANES):
        cols = slice(c * LANES, (c + 1) * LANES)
        val = values[:, cols].astype(jnp.bfloat16).astype(jnp.float32)
        vv_ref[0, :, cols] = val.astype(jnp.bfloat16)
        vv_ref[1, :, cols] = pltpu.roll(val, head_dim, 1).astype(jnp.bfloat16)


def qkv_call(x_rows, gain, w_qkv, cos_tab, sin_tab, head_dim, q_cols, k_cols):
    tokens, width = x_rows.shape
    rows = QKV_ROWS
    return pl.pallas_call(
        functools.partial(qkv_kernel, head_dim, q_cols, k_cols),
        grid=(tokens // rows,),
        in_specs=[
            pl.BlockSpec((rows, width), lambda i: (i, 0)),
            resident((1, width), lambda i: (0, 0)),
            resident((width, q_cols + 2 * k_cols), lambda i: (0, 0)),
            pl.BlockSpec((rows, LANES), lambda i: (i, 0)),
            pl.BlockSpec((rows, LANES), lambda i: (i, 0)),
        ],
        out_specs=[
            pl.BlockSpec((rows, q_cols), lambda i: (i, 0)),
            pl.BlockSpec((2, rows, k_cols), lambda i: (0, i, 0)),
            pl.BlockSpec((2, rows, k_cols), lambda i: (0, i, 0)),
        ],
        out_shape=[
            jax.ShapeDtypeStruct((tokens, q_cols), jnp.bfloat16),
            jax.ShapeDtypeStruct((2, tokens, k_cols), jnp.bfloat16),
            jax.ShapeDtypeStruct((2, tokens, k_cols), jnp.bfloat16),
        ],
        compiler_params=pltpu.CompilerParams(vmem_limit_bytes=BIG_VMEM),
        cost_estimate=pl.CostEstimate(flops=2 * tokens * width * (q_cols + 2 * k_cols), bytes_accessed=tokens * width * 10, transcendentals=0),
        name='qkv_rope',
    )(x_rows, gain, w_qkv, cos_tab, sin_tab)


def attend_kernel(head_dim, q_ref, ka_ref, kb_ref, va_ref, vb_ref, o_ref, q_buf, s_buf):
    rows = q_ref.shape[0]
    half = rows // 2
    tokens = ka_ref.shape[1]
    step = pl.program_id(1)
    lane = lax.broadcasted_iota(jnp.int32, (rows, LANES), 1)
    low = lane < head_dim
    query = q_ref[...].astype(jnp.float32) * (head_dim ** -0.5)
    zero = jnp.zeros_like(query)
    q_buf[0] = jnp.where(low, query, zero).astype(jnp.bfloat16)
    q_buf[1] = jnp.where(low, zero, query).astype(jnp.bfloat16)
    key_refs = (ka_ref, kb_ref)
    val_refs = (va_ref, vb_ref)

    def fold(op, tile, out):
        for g in range(tile.shape[1] // LANES):
            part = tile[:, g * LANES:(g + 1) * LANES]
            out = part if out is None else op(out, part)
        return out

    def run_case(case):
        chains = [dict(head=head, part=part, top=None, total=None, out=None) for part in range(2) for head in range(2)]
        for chain in chains:
            diag = (2 * case + chain['part']) * half
            pieces = []
            start = 0
            while start < diag:
                width = min(rows, diag - start)
                pieces.append((start, width, False))
                start += width
            chain['pieces'] = pieces + [(diag, half, True)]

        def scores(slot, chain, piece):
            start, width, masked = piece
            own = q_buf[chain['head'], chain['part'] * half:(chain['part'] + 1) * half, :]
            tile = f32dot_t(own, key_refs[chain['head']][0, start:start + width, :])
            if masked:
                row_id = lax.broadcasted_iota(jnp.int32, (half, width), 0)
                col_id = lax.broadcasted_iota(jnp.int32, (half, width), 1)
                tile = jnp.where(row_id >= col_id, tile, -1e30)
            s_buf[slot, :, start:start + width] = tile
            chain['top'] = fold(jnp.maximum, tile, chain['top'])

        def exps(slot, chain, piece):
            start, width, _ = piece
            tile = jnp.exp(s_buf[slot, :, start:start + width] - chain['row_max'])
            s_buf[slot, :, start:start + width] = tile
            chain['total'] = fold(jnp.add, tile, chain['total'])

        def mixes(slot, chain, piece):
            start, width, _ = piece
            prob = (s_buf[slot, :, start:start + width] * chain['inv']).astype(jnp.bfloat16)
            part = f32dot(prob, val_refs[chain['head']][0, start:start + width, :])
            chain['out'] = part if chain['out'] is None else chain['out'] + part

        count = len(chains)
        for slot in range(count + 2):
            work = []
            if slot < count:
                work.append((scores, slot))
            if 0 <= slot - 1 < count:
                chain = chains[slot - 1]
                chain['row_max'] = jnp.max(chain['top'], axis=-1, keepdims=True)
                work.append((exps, slot - 1))
            if 0 <= slot - 2 < count:
                chain = chains[slot - 2]
                chain['inv'] = 1.0 / jnp.sum(chain['total'], axis=-1, keepdims=True)
                work.append((mixes, slot - 2))
            for j in range(max(len(chains[i]['pieces']) for _, i in work)):
                for stage, i in work:
                    if j < len(chains[i]['pieces']):
                        stage(i, chains[i], chains[i]['pieces'][j])
        low_half = low[:half]
        for part in range(2):
            first, second = chains[2 * part]['out'], chains[2 * part + 1]['out']
            o_ref[part * half:(part + 1) * half, :] = jnp.where(low_half, first, second).astype(jnp.bfloat16)

    for case in range(tokens // rows):
        pl.when(step == case)(functools.partial(run_case, case))


def attend_call(query, keys, values, head_dim):
    tokens, q_cols = query.shape
    kv_heads = keys.shape[2] // head_dim
    rows = min(ATT_ROWS, tokens)
    per_tile = LANES // head_dim
    kv_block = (1, tokens, LANES)
    same = lambda h, i: (h % per_tile, 0, h // per_tile)
    other = lambda h, i: (1 - h % per_tile, 0, h // per_tile)
    return pl.pallas_call(
        functools.partial(attend_kernel, head_dim),
        grid=(kv_heads, tokens // rows),
        in_specs=[
            pl.BlockSpec((rows, LANES), lambda h, i: (i, h)),
            pl.BlockSpec(kv_block, same),
            pl.BlockSpec(kv_block, other),
            pl.BlockSpec(kv_block, same),
            pl.BlockSpec(kv_block, other),
        ],
        out_specs=pl.BlockSpec((rows, LANES), lambda h, i: (i, h)),
        out_shape=jax.ShapeDtypeStruct((tokens, q_cols), jnp.bfloat16),
        scratch_shapes=[
            pltpu.VMEM((2, rows, LANES), jnp.bfloat16),
            pltpu.VMEM((4, rows // 2, tokens), jnp.float32),
        ],
        compiler_params=pltpu.CompilerParams(vmem_limit_bytes=BIG_VMEM),
        cost_estimate=pl.CostEstimate(flops=8 * tokens * tokens * q_cols, bytes_accessed=tokens * q_cols * 12, transcendentals=tokens * tokens * q_cols // LANES),
        name='attend',
    )(query, keys, keys, values, values)


def out_kernel(mixed_ref, w_ref, x_ref, gain_ref, h_ref, u_ref):
    hidden = (x_ref[...].astype(jnp.float32) + f32dot(mixed_ref[...], w_ref[...])).astype(jnp.bfloat16)
    h_ref[...] = hidden
    u_ref[...] = rms_rows(hidden.astype(jnp.float32), gain_ref[...].astype(jnp.float32))


def out_call(mixed, w_attn, x_rows, gain):
    tokens, width = x_rows.shape
    rows = OUT_ROWS
    block = pl.BlockSpec((rows, width), lambda i: (i, 0))
    return pl.pallas_call(
        out_kernel,
        grid=(tokens // rows,),
        in_specs=[
            pl.BlockSpec((rows, mixed.shape[1]), lambda i: (i, 0)),
            resident((mixed.shape[1], width), lambda i: (0, w_attn.shape[1] // width - 1)),
            block,
            resident((1, width), lambda i: (0, 0)),
        ],
        out_specs=[block, block],
        out_shape=[jax.ShapeDtypeStruct((tokens, width), jnp.bfloat16)] * 2,
        compiler_params=pltpu.CompilerParams(vmem_limit_bytes=BIG_VMEM),
        cost_estimate=pl.CostEstimate(flops=2 * tokens * width * mixed.shape[1], bytes_accessed=tokens * width * 10, transcendentals=0),
        name='out_proj',
    )(mixed, w_attn, x_rows, gain)


def moe_kernel(first_expert, is_first, is_last, count_ref, u_ref, gate_ref, slot_ref, slot_row_ref, w_ref, *rest):
    rest = list(rest)
    acc_in = None if is_first else rest.pop(0)
    h_ref = rest.pop(0) if is_last else None
    out_ref, acc, prior, sems = rest
    step = pl.program_id(0)
    expert = first_expert + step
    shards, _, _, depth, inner = w_ref.shape
    full = shards * depth
    tokens = u_ref.shape[0]
    count = count_ref[expert]

    def span(blk):
        return pl.ds(pl.multiple_of(blk * MOE_ROWS, MOE_ROWS), MOE_ROWS)

    def matrix(i):
        return w_ref[:, i, 0].reshape(full, inner)

    def column(ref, rows):
        vals = ref[rows, :]
        lane = lax.broadcasted_iota(jnp.int32, vals.shape, 1)
        return jnp.sum(jnp.where(lane == expert, vals, jnp.zeros_like(vals)), axis=-1, keepdims=True)

    def middle(in_rows):
        return (jax.nn.silu(f32dot(in_rows, matrix(0))) * f32dot(in_rows, matrix(1))).astype(jnp.bfloat16)

    @pl.when(step == 0)
    def _():
        if not is_first:
            pltpu.make_async_copy(acc_in, prior, sems.at[0]).start()

        @pl.loop(0, tokens // MOE_ROWS)
        def _(blk):
            acc[span(blk), :] = jnp.zeros((MOE_ROWS, acc.shape[1]), jnp.float32)

    @pl.when(count > FEW_ROWS)
    def _():
        @pl.loop(0, tokens // (MOE_PAIR * MOE_ROWS))
        def _(trip):
            spans = [span(trip * MOE_PAIR + i) for i in range(MOE_PAIR)]
            mids = [middle(u_ref[rows, :]) for rows in spans]
            for rows, mid in zip(spans, mids):
                y_rows = f32dot_t(mid, matrix(2)).astype(jnp.bfloat16).astype(jnp.float32)
                weight = column(gate_ref, rows)
                acc[rows, :] += jnp.where(weight > 0, weight * y_rows, 0.0)

    @pl.when((count > 0) & (count <= FEW_ROWS))
    def _():
        place = lax.broadcasted_iota(jnp.int32, (FEW_ROWS, tokens), 0)
        pick = jnp.where(slot_row_ref[pl.ds(expert, 1), :] == place, 1.0, 0.0).astype(jnp.bfloat16)
        in_rows = f32dot(pick, u_ref[...]).astype(jnp.bfloat16)
        y_rows = f32dot_t(middle(in_rows), matrix(2)).astype(jnp.bfloat16)

        @pl.loop(0, tokens // MOE_ROWS)
        def _(blk):
            rows = span(blk)
            place = lax.broadcasted_iota(jnp.int32, (MOE_ROWS, FEW_ROWS), 1).astype(jnp.float32)
            spread = jnp.where(column(slot_ref, rows) == place, column(gate_ref, rows), 0.0).astype(jnp.bfloat16)
            acc[rows, :] += f32dot(spread, y_rows)

    @pl.when(step == pl.num_programs(0) - 1)
    def _():
        if not is_first:
            pltpu.make_async_copy(acc_in, prior, sems.at[0]).wait()

        def out_copy(blk):
            return pltpu.make_async_copy(acc.at[span(blk), :], out_ref.at[span(blk), :], sems.at[1])

        @pl.loop(0, tokens // MOE_ROWS)
        def _(blk):
            rows = span(blk)
            total = acc[rows, :] if is_first else acc[rows, :] + prior[rows, :]
            if is_last:
                out_ref[rows, :] = (h_ref[rows, :].astype(jnp.float32) + total).astype(jnp.bfloat16)
            else:
                if not is_first:
                    acc[rows, :] = total
                out_copy(blk).start()

        if not is_last:
            @pl.loop(0, tokens // MOE_ROWS)
            def _(blk):
                out_copy(blk).wait()


def moe_call(u_rows, routing, weights, acc, h_rows, first_expert, is_last):
    tokens, width = u_rows.shape
    shards, parts, count, depth, inner = weights.shape
    is_first = acc is None
    whole = lambda e: (0, 0)
    counts, gates, slots, slot_rows = routing
    args = [counts, u_rows, gates, slots, slot_rows, weights]
    in_specs = [
        pl.BlockSpec(memory_space=pltpu.SMEM),
        resident((tokens, width), whole),
        resident(gates.shape, whole),
        resident(slots.shape, whole),
        resident(slot_rows.shape, whole),
        pl.BlockSpec((shards, parts, 1, depth, inner), lambda e: (0, 0, e, 0, 0)),
    ]
    if not is_first:
        args.append(acc)
        in_specs.append(pl.BlockSpec(memory_space=pl.ANY))
    if is_last:
        args.append(h_rows)
        in_specs.append(resident((tokens, width), whole))
        out_spec = resident((tokens, width), whole)
        out_shape = jax.ShapeDtypeStruct((tokens, width), jnp.bfloat16)
    else:
        out_spec = pl.BlockSpec(memory_space=pl.ANY)
        out_shape = jax.ShapeDtypeStruct((tokens, width), jnp.float32)
    prior_shape = (8, LANES) if is_first else (tokens, width)
    return pl.pallas_call(
        functools.partial(moe_kernel, first_expert, is_first, is_last),
        grid=(count,),
        in_specs=in_specs,
        out_specs=out_spec,
        out_shape=out_shape,
        scratch_shapes=[pltpu.VMEM((tokens, width), jnp.float32), pltpu.VMEM(prior_shape, jnp.float32), pltpu.SemaphoreType.DMA((2,))],
        compiler_params=pltpu.CompilerParams(vmem_limit_bytes=BIG_VMEM),
        cost_estimate=pl.CostEstimate(flops=6 * tokens * width * inner * count, bytes_accessed=2 * weights.size + 16 * tokens * width, transcendentals=tokens * inner * count),
        name='moe_part',
    )(*args)


def routing_tables(expert_ids, slot_ids, counts, weights):
    tokens, choices = expert_ids.shape
    experts = counts.shape[0]
    limits = jnp.pad(counts, (0, LANES - experts))[None, :]
    lane = lax.broadcasted_iota(jnp.int32, (tokens, LANES), 1)
    row = lax.broadcasted_iota(jnp.int32, (experts, tokens), 0)
    gates = jnp.zeros((tokens, LANES), jnp.float32)
    slots = jnp.full((tokens, LANES), -1.0, jnp.float32)
    slot_rows = jnp.full((experts, tokens), -1, jnp.int32)
    for k in range(choices):
        ids, slot = expert_ids[:, k], slot_ids[:, k]
        kept = (ids[:, None] == lane) & (slot[:, None] < limits)
        gates = jnp.where(kept, weights[:, k:k + 1].astype(jnp.float32), gates)
        slots = jnp.where(kept, slot[:, None].astype(jnp.float32), slots)
        slot_rows = jnp.where((ids[None, :] == row) & (slot[None, :] < counts[:, None]), slot[None, :], slot_rows)
    return counts, gates, slots, slot_rows


def rotary_tables(tokens, head_dim):
    half_dim = head_dim // 2
    lane = jnp.arange(LANES)
    inv_freq = 10000.0 ** (-(lane % half_dim).astype(jnp.float32) / half_dim)
    angles = jnp.arange(tokens, dtype=jnp.float32)[:, None] * inv_freq[None, :]
    sign = jnp.where(lane % head_dim < half_dim, -1.0, 1.0)
    return jnp.cos(angles), jnp.sin(angles) * sign[None, :]


def local_layer(x_rows, w_attn, attn_gain, moe_gain, expert_parts, routing, tables, head_dim, q_cols, k_cols):
    query, keys, values = qkv_call(x_rows, attn_gain, w_attn, *tables, head_dim, q_cols, k_cols)
    mixed = attend_call(query, keys, values, head_dim)
    h_rows, u_rows = out_call(mixed, w_attn, x_rows, moe_gain)
    acc = None
    first = 0
    for i, part in enumerate(expert_parts):
        acc = moe_call(u_rows, routing, part, acc, h_rows, first, i == len(expert_parts) - 1)
        first += part.shape[2]
    return acc


def shares_of(experts):
    total = sum(SHARES)
    sizes = [experts * share // total for share in SHARES[1:]]
    return [experts - sum(sizes)] + sizes


def solution(mesh):
    row_spec = P(('data', 'ep'))

    def device_step(x_in, w_query, w_keyval, w_out, attn_gain, moe_gain, w_gate, w_up, w_down, expert_ids, slot_ids, fill_counts, route_weight):
        batch_loc, seq_len, model_dim = x_in.shape
        rows_loc, num_heads, head_dim = w_query.shape
        q_cols = num_heads * head_dim
        k_cols = w_keyval.shape[1] // 2 * head_dim
        experts = w_gate.shape[0]
        w_local = jnp.concatenate([w_query.reshape(rows_loc, q_cols), w_keyval.reshape(rows_loc, 2 * k_cols), w_out], axis=1)
        w_attn = lax.all_gather(w_local, 'ep', axis=0, tiled=True)
        mats = (w_gate, w_up, jnp.swapaxes(w_down, 1, 2))
        stacks = []
        first = 0
        for size in shares_of(experts):
            stacks.append(jnp.stack([mat[first:first + size] for mat in mats]))
            first += size
        tables = rotary_tables(seq_len, head_dim)
        routing = [routing_tables(expert_ids[b], slot_ids[b], fill_counts[0], route_weight[b]) for b in range(batch_loc)]
        gains = (attn_gain[None, :], moe_gain[None, :])
        stacks, tables, routing, gains, w_attn = lax.optimization_barrier((stacks, tables, routing, gains, w_attn))
        expert_parts = [lax.all_gather(part, 'ep', axis=0, tiled=False) for part in stacks]
        outs = []
        for b in range(batch_loc):
            outs.append(local_layer(x_in[b], w_attn, *gains, expert_parts, routing[b], tables, head_dim, q_cols, k_cols))
        return jnp.stack(outs)

    in_specs = (row_spec, P('ep'), P('ep'), P('ep'), P(), P(), P(None, 'ep'), P(None, 'ep'), P(None, None, 'ep'), row_spec, row_spec, row_spec, row_spec)
    return jax.shard_map(device_step, mesh=mesh, in_specs=in_specs, out_specs=row_spec, check_vma=False)
```

```python
import functools

import jax
import jax.numpy as jnp
from jax import lax
from jax.experimental import pallas as pl
from jax.experimental.pallas import tpu as pltpu
from jax.sharding import PartitionSpec as P

LANES = 128
QKV_ROWS = 256
ATT_ROWS = 512
OUT_ROWS = 256
MOE_ROWS = 512
MOE_PAIR = 2
FEW_ROWS = 256
SPREAD_ROWS = 256
PASS_ROWS = 64
MATRICES = 3
SHARES = (4, 14, 9, 5)
BIG_VMEM = 60 * 1024 * 1024


def f32dot(lhs, rhs):
    return jnp.dot(lhs, rhs, preferred_element_type=jnp.float32)


def f32dot_t(lhs, rhs):
    return lax.dot_general(lhs, rhs, (((1,), (1,)), ((), ())), preferred_element_type=jnp.float32)


def rms_rows(v32, gain):
    scale = lax.rsqrt(jnp.mean(v32 * v32, axis=-1, keepdims=True) + 1e-6)
    return (v32 * scale * gain).astype(jnp.bfloat16)


def resident(shape, index_map):
    return pl.BlockSpec(shape, index_map, pipeline_mode=pl.Buffered(1))


def qkv_kernel(head_dim, q_cols, k_cols, x_ref, gain_ref, w_ref, cos_ref, sin_ref, q_ref, kk_ref, vv_ref):
    half_dim = head_dim // 2
    normed = rms_rows(x_ref[...].astype(jnp.float32), gain_ref[...].astype(jnp.float32))
    cos_tab = cos_ref[...]
    sin_tab = sin_ref[...]
    rows = x_ref.shape[0]
    lane = lax.broadcasted_iota(jnp.int32, (rows, LANES), 1)
    low_half = lax.rem(lane, head_dim) < half_dim

    def rotated(vals):
        v32 = vals.astype(jnp.bfloat16).astype(jnp.float32)
        other = jnp.where(low_half, pltpu.roll(v32, LANES - half_dim, 1), pltpu.roll(v32, half_dim, 1))
        return v32 * cos_tab + other * sin_tab

    shards, _, depth, inner = w_ref.shape

    def product(block):
        return f32dot(normed, w_ref[:, block].reshape(shards * depth, inner))

    chunks = inner // LANES
    for block in range(q_cols // inner):
        query = product(block)
        for c in range(chunks):
            cols = slice(block * inner + c * LANES, block * inner + (c + 1) * LANES)
            q_ref[:, cols] = rotated(query[:, c * LANES:(c + 1) * LANES]).astype(jnp.bfloat16)
    for block in range(k_cols // inner):
        keys = product(q_cols // inner + block)
        values = product((q_cols + k_cols) // inner + block)
        for c in range(chunks):
            own = slice(c * LANES, (c + 1) * LANES)
            cols = slice(block * inner + c * LANES, block * inner + (c + 1) * LANES)
            rot = rotated(keys[:, own]).astype(jnp.bfloat16).astype(jnp.float32)
            kk_ref[0, :, cols] = rot.astype(jnp.bfloat16)
            kk_ref[1, :, cols] = pltpu.roll(rot, head_dim, 1).astype(jnp.bfloat16)
            val = values[:, own].astype(jnp.bfloat16).astype(jnp.float32)
            vv_ref[0, :, cols] = val.astype(jnp.bfloat16)
            vv_ref[1, :, cols] = pltpu.roll(val, head_dim, 1).astype(jnp.bfloat16)


def qkv_call(x_rows, gain, blocks, cos_tab, sin_tab, head_dim, q_cols, k_cols):
    tokens, width = x_rows.shape
    shards, _, depth, inner = blocks.shape
    rows = QKV_ROWS
    return pl.pallas_call(
        functools.partial(qkv_kernel, head_dim, q_cols, k_cols),
        grid=(tokens // rows,),
        in_specs=[
            pl.BlockSpec((rows, width), lambda i: (i, 0)),
            resident((1, width), lambda i: (0, 0)),
            resident((shards, (q_cols + 2 * k_cols) // inner, depth, inner), lambda i: (0, 0, 0, 0)),
            pl.BlockSpec((rows, LANES), lambda i: (i, 0)),
            pl.BlockSpec((rows, LANES), lambda i: (i, 0)),
        ],
        out_specs=[
            pl.BlockSpec((rows, q_cols), lambda i: (i, 0)),
            pl.BlockSpec((2, rows, k_cols), lambda i: (0, i, 0)),
            pl.BlockSpec((2, rows, k_cols), lambda i: (0, i, 0)),
        ],
        out_shape=[
            jax.ShapeDtypeStruct((tokens, q_cols), jnp.bfloat16),
            jax.ShapeDtypeStruct((2, tokens, k_cols), jnp.bfloat16),
            jax.ShapeDtypeStruct((2, tokens, k_cols), jnp.bfloat16),
        ],
        compiler_params=pltpu.CompilerParams(vmem_limit_bytes=BIG_VMEM),
        cost_estimate=pl.CostEstimate(flops=2 * tokens * width * (q_cols + 2 * k_cols), bytes_accessed=tokens * width * 10, transcendentals=0),
        name='qkv_rope',
    )(x_rows, gain, blocks, cos_tab, sin_tab)


def attend_kernel(head_dim, q_ref, ka_ref, kb_ref, va_ref, vb_ref, o_ref, q_buf, s_buf):
    rows = q_ref.shape[0]
    half = rows // 2
    tokens = ka_ref.shape[1]
    step = pl.program_id(1)
    lane = lax.broadcasted_iota(jnp.int32, (rows, LANES), 1)
    low = lane < head_dim
    query = q_ref[...].astype(jnp.float32) * (head_dim ** -0.5)
    zero = jnp.zeros_like(query)
    q_buf[0] = jnp.where(low, query, zero).astype(jnp.bfloat16)
    q_buf[1] = jnp.where(low, zero, query).astype(jnp.bfloat16)
    key_refs = (ka_ref, kb_ref)
    val_refs = (va_ref, vb_ref)

    def fold(op, tile, out):
        for g in range(tile.shape[1] // LANES):
            part = tile[:, g * LANES:(g + 1) * LANES]
            out = part if out is None else op(out, part)
        return out

    def run_case(case):
        chains = [dict(head=head, part=part, top=None, total=None, out=None) for part in range(2) for head in range(2)]
        for chain in chains:
            diag = (2 * case + chain['part']) * half
            pieces = []
            start = 0
            while start < diag:
                width = min(rows, diag - start)
                pieces.append((start, width, False))
                start += width
            chain['pieces'] = pieces + [(diag, half, True)]

        def scores(slot, chain, piece):
            start, width, masked = piece
            own = q_buf[chain['head'], chain['part'] * half:(chain['part'] + 1) * half, :]
            tile = f32dot_t(own, key_refs[chain['head']][0, start:start + width, :])
            if masked:
                row_id = lax.broadcasted_iota(jnp.int32, (half, width), 0)
                col_id = lax.broadcasted_iota(jnp.int32, (half, width), 1)
                tile = jnp.where(row_id >= col_id, tile, -1e30)
            s_buf[slot, :, start:start + width] = tile
            chain['top'] = fold(jnp.maximum, tile, chain['top'])

        def exps(slot, chain, piece):
            start, width, _ = piece
            tile = jnp.exp(s_buf[slot, :, start:start + width] - chain['row_max'])
            s_buf[slot, :, start:start + width] = tile
            chain['total'] = fold(jnp.add, tile, chain['total'])

        def mixes(slot, chain, piece):
            start, width, _ = piece
            prob = (s_buf[slot, :, start:start + width] * chain['inv']).astype(jnp.bfloat16)
            part = f32dot(prob, val_refs[chain['head']][0, start:start + width, :])
            chain['out'] = part if chain['out'] is None else chain['out'] + part

        count = len(chains)
        for slot in range(count + 2):
            work = []
            if slot < count:
                work.append((scores, slot))
            if 0 <= slot - 1 < count:
                chain = chains[slot - 1]
                chain['row_max'] = jnp.max(chain['top'], axis=-1, keepdims=True)
                work.append((exps, slot - 1))
            if 0 <= slot - 2 < count:
                chain = chains[slot - 2]
                chain['inv'] = 1.0 / jnp.sum(chain['total'], axis=-1, keepdims=True)
                work.append((mixes, slot - 2))
            for j in range(max(len(chains[i]['pieces']) for _, i in work)):
                for stage, i in work:
                    if j < len(chains[i]['pieces']):
                        stage(i, chains[i], chains[i]['pieces'][j])
        low_half = low[:half]
        for part in range(2):
            first, second = chains[2 * part]['out'], chains[2 * part + 1]['out']
            o_ref[part * half:(part + 1) * half, :] = jnp.where(low_half, first, second).astype(jnp.bfloat16)

    for case in range(tokens // rows):
        pl.when(step == case)(functools.partial(run_case, case))


def attend_call(query, keys, values, head_dim):
    tokens, q_cols = query.shape
    kv_heads = keys.shape[2] // head_dim
    rows = min(ATT_ROWS, tokens)
    per_tile = LANES // head_dim
    kv_block = (1, tokens, LANES)
    same = lambda h, i: (h % per_tile, 0, h // per_tile)
    other = lambda h, i: (1 - h % per_tile, 0, h // per_tile)
    return pl.pallas_call(
        functools.partial(attend_kernel, head_dim),
        grid=(kv_heads, tokens // rows),
        in_specs=[
            pl.BlockSpec((rows, LANES), lambda h, i: (i, h)),
            pl.BlockSpec(kv_block, same),
            pl.BlockSpec(kv_block, other),
            pl.BlockSpec(kv_block, same),
            pl.BlockSpec(kv_block, other),
        ],
        out_specs=pl.BlockSpec((rows, LANES), lambda h, i: (i, h)),
        out_shape=jax.ShapeDtypeStruct((tokens, q_cols), jnp.bfloat16),
        scratch_shapes=[
            pltpu.VMEM((2, rows, LANES), jnp.bfloat16),
            pltpu.VMEM((4, rows // 2, tokens), jnp.float32),
        ],
        compiler_params=pltpu.CompilerParams(vmem_limit_bytes=BIG_VMEM),
        cost_estimate=pl.CostEstimate(flops=8 * tokens * tokens * q_cols, bytes_accessed=tokens * q_cols * 12, transcendentals=tokens * tokens * q_cols // LANES),
        name='attend',
    )(query, keys, keys, values, values)


def out_kernel(mixed_ref, w_ref, x_ref, gain_ref, h_ref, u_ref):
    shards, parts, depth, inner = w_ref.shape
    mixed = mixed_ref[...]
    attn_out = jnp.concatenate([f32dot(mixed, w_ref[:, i].reshape(shards * depth, inner)) for i in range(parts)], axis=1)
    hidden = (x_ref[...].astype(jnp.float32) + attn_out).astype(jnp.bfloat16)
    h_ref[...] = hidden
    u_ref[...] = rms_rows(hidden.astype(jnp.float32), gain_ref[...].astype(jnp.float32))


def out_call(mixed, blocks, first_block, x_rows, gain):
    tokens, width = x_rows.shape
    shards, _, depth, inner = blocks.shape
    parts = width // inner
    rows = OUT_ROWS
    block = pl.BlockSpec((rows, width), lambda i: (i, 0))
    return pl.pallas_call(
        out_kernel,
        grid=(tokens // rows,),
        in_specs=[
            pl.BlockSpec((rows, mixed.shape[1]), lambda i: (i, 0)),
            resident((shards, parts, depth, inner), lambda i: (0, first_block // parts, 0, 0)),
            block,
            resident((1, width), lambda i: (0, 0)),
        ],
        out_specs=[block, block],
        out_shape=[jax.ShapeDtypeStruct((tokens, width), jnp.bfloat16)] * 2,
        compiler_params=pltpu.CompilerParams(vmem_limit_bytes=BIG_VMEM),
        cost_estimate=pl.CostEstimate(flops=2 * tokens * width * mixed.shape[1], bytes_accessed=tokens * width * 10, transcendentals=0),
        name='out_proj',
    )(mixed, blocks, x_rows, gain)


def moe_kernel(first_expert, is_first, is_last, count_ref, u_ref, gate_ref, slot_ref, slot_row_ref, w1_ref, w3_ref, w2_ref, *rest):
    rest = list(rest)
    acc_in = None if is_first else rest.pop(0)
    h_ref = rest.pop(0) if is_last else None
    out_ref, acc, prior, sems = rest
    step = pl.program_id(0)
    expert = first_expert + step
    shards, _, depth, inner = w1_ref.shape
    full = shards * depth
    mat_refs = (w1_ref, w3_ref, w2_ref)
    pair = 1 if is_first else MOE_PAIR
    few = 0 if is_first else FEW_ROWS
    tokens = u_ref.shape[0]
    count = count_ref[expert]

    def span(blk):
        return pl.ds(pl.multiple_of(blk * MOE_ROWS, MOE_ROWS), MOE_ROWS)

    def strip(blk):
        return pl.ds(pl.multiple_of(blk * PASS_ROWS, PASS_ROWS), PASS_ROWS)

    def matrix(i):
        return mat_refs[i][:, 0].reshape(full, inner)

    def column(ref, rows):
        vals = ref[rows, :]
        lane = lax.broadcasted_iota(jnp.int32, vals.shape, 1)
        return jnp.sum(jnp.where(lane == expert, vals, jnp.zeros_like(vals)), axis=-1, keepdims=True)

    def middle(in_rows):
        return (jax.nn.silu(f32dot(in_rows, matrix(0))) * f32dot(in_rows, matrix(1))).astype(jnp.bfloat16)

    @pl.when(step == 0)
    def _():
        if not is_first:
            pltpu.make_async_copy(acc_in, prior, sems.at[0]).start()

        @pl.loop(0, tokens // PASS_ROWS)
        def _(blk):
            acc[strip(blk), :] = jnp.zeros((PASS_ROWS, acc.shape[1]), jnp.float32)

    @pl.when(count > few)
    def _():
        @pl.loop(0, tokens // (pair * MOE_ROWS))
        def _(trip):
            spans = [span(trip * pair + i) for i in range(pair)]
            mids = [middle(u_ref[rows, :]) for rows in spans]
            for rows, mid in zip(spans, mids):
                y_rows = f32dot_t(mid, matrix(2)).astype(jnp.bfloat16).astype(jnp.float32)
                weight = column(gate_ref, rows)
                acc[rows, :] += jnp.where(weight > 0, weight * y_rows, 0.0)

    def few_step():
        place = lax.broadcasted_iota(jnp.int32, (few, tokens), 0)
        pick = jnp.where(slot_row_ref[pl.ds(expert, 1), :] == place, 1.0, 0.0).astype(jnp.bfloat16)
        in_rows = f32dot(pick, u_ref[...]).astype(jnp.bfloat16)
        y_rows = f32dot_t(middle(in_rows), matrix(2)).astype(jnp.bfloat16)

        @pl.loop(0, tokens // SPREAD_ROWS)
        def _(blk):
            rows = pl.ds(pl.multiple_of(blk * SPREAD_ROWS, SPREAD_ROWS), SPREAD_ROWS)
            place = lax.broadcasted_iota(jnp.int32, (SPREAD_ROWS, few), 1).astype(jnp.float32)
            spread = jnp.where(column(slot_ref, rows) == place, column(gate_ref, rows), 0.0).astype(jnp.bfloat16)
            acc[rows, :] += f32dot(spread, y_rows)

    if few:
        pl.when((count > 0) & (count <= few))(few_step)

    @pl.when(step == pl.num_programs(0) - 1)
    def _():
        if not is_first:
            pltpu.make_async_copy(acc_in, prior, sems.at[0]).wait()

        def out_copy(blk):
            return pltpu.make_async_copy(acc.at[strip(blk), :], out_ref.at[strip(blk), :], sems.at[1])

        @pl.loop(0, tokens // PASS_ROWS)
        def _(blk):
            rows = strip(blk)
            total = acc[rows, :] if is_first else acc[rows, :] + prior[rows, :]
            if is_last:
                out_ref[rows, :] = (h_ref[rows, :].astype(jnp.float32) + total).astype(jnp.bfloat16)
            else:
                if not is_first:
                    acc[rows, :] = total
                out_copy(blk).start()

        if not is_last:
            @pl.loop(0, tokens // PASS_ROWS)
            def _(blk):
                out_copy(blk).wait()


def moe_call(u_rows, routing, blocks, first_block, acc, h_rows, first_expert, is_last):
    tokens, width = u_rows.shape
    shards, total, depth, inner = blocks.shape
    count = (total - first_block) // MATRICES
    is_first = acc is None
    whole = lambda e: (0, 0)
    counts, gates, slots, slot_rows = routing
    args = [counts, u_rows, gates, slots, slot_rows, blocks, blocks, blocks]
    in_specs = [
        pl.BlockSpec(memory_space=pltpu.SMEM),
        resident((tokens, width), whole),
        resident(gates.shape, whole),
        resident(slots.shape, whole),
        resident(slot_rows.shape, whole),
    ]
    for i in range(MATRICES):
        in_specs.append(pl.BlockSpec((shards, 1, depth, inner), lambda e, i=i: (0, first_block + i * count + e, 0, 0)))
    if not is_first:
        args.append(acc)
        in_specs.append(pl.BlockSpec(memory_space=pl.ANY))
    if is_last:
        args.append(h_rows)
        in_specs.append(resident((tokens, width), whole))
        out_spec = resident((tokens, width), whole)
        out_shape = jax.ShapeDtypeStruct((tokens, width), jnp.bfloat16)
    else:
        out_spec = pl.BlockSpec(memory_space=pl.ANY)
        out_shape = jax.ShapeDtypeStruct((tokens, width), jnp.float32)
    prior_shape = (8, LANES) if is_first else (tokens, width)
    return pl.pallas_call(
        functools.partial(moe_kernel, first_expert, is_first, is_last),
        grid=(count,),
        in_specs=in_specs,
        out_specs=out_spec,
        out_shape=out_shape,
        scratch_shapes=[pltpu.VMEM((tokens, width), jnp.float32), pltpu.VMEM(prior_shape, jnp.float32), pltpu.SemaphoreType.DMA((2,))],
        compiler_params=pltpu.CompilerParams(vmem_limit_bytes=BIG_VMEM),
        cost_estimate=pl.CostEstimate(flops=6 * tokens * width * inner * count, bytes_accessed=2 * blocks.size + 16 * tokens * width, transcendentals=tokens * inner * count),
        name='moe_part',
    )(*args)


def routing_tables(expert_ids, slot_ids, counts, weights):
    tokens, choices = expert_ids.shape
    experts = counts.shape[0]
    limits = jnp.pad(counts, (0, LANES - experts))[None, :]
    lane = lax.broadcasted_iota(jnp.int32, (tokens, LANES), 1)
    row = lax.broadcasted_iota(jnp.int32, (experts, tokens), 0)
    gates = jnp.zeros((tokens, LANES), jnp.float32)
    slots = jnp.full((tokens, LANES), -1.0, jnp.float32)
    slot_rows = jnp.full((experts, tokens), -1, jnp.int32)
    for k in range(choices):
        ids, slot = expert_ids[:, k], slot_ids[:, k]
        kept = (ids[:, None] == lane) & (slot[:, None] < limits)
        gates = jnp.where(kept, weights[:, k:k + 1].astype(jnp.float32), gates)
        slots = jnp.where(kept, slot[:, None].astype(jnp.float32), slots)
        slot_rows = jnp.where((ids[None, :] == row) & (slot[None, :] < counts[:, None]), slot[None, :], slot_rows)
    return counts, gates, slots, slot_rows


def rotary_tables(tokens, head_dim):
    half_dim = head_dim // 2
    lane = jnp.arange(LANES)
    inv_freq = 10000.0 ** (-(lane % half_dim).astype(jnp.float32) / half_dim)
    angles = jnp.arange(tokens, dtype=jnp.float32)[:, None] * inv_freq[None, :]
    sign = jnp.where(lane % head_dim < half_dim, -1.0, 1.0)
    return jnp.cos(angles), jnp.sin(angles) * sign[None, :]


def local_layer(x_rows, attn_gain, moe_gain, parts, attn_blocks, routing, tables, head_dim, q_cols, k_cols):
    query, keys, values = qkv_call(x_rows, attn_gain, parts[0], *tables, head_dim, q_cols, k_cols)
    mixed = attend_call(query, keys, values, head_dim)
    inner = parts[0].shape[-1]
    h_rows, u_rows = out_call(mixed, parts[0], (q_cols + 2 * k_cols) // inner, x_rows, moe_gain)
    acc = None
    expert = 0
    for i, blocks in enumerate(parts):
        first_block = 0 if i else attn_blocks
        acc = moe_call(u_rows, routing, blocks, first_block, acc, h_rows, expert, i == len(parts) - 1)
        expert += (blocks.shape[1] - first_block) // MATRICES
    return acc


def shares_of(experts):
    total = sum(SHARES)
    sizes = [experts * share // total for share in SHARES[1:]]
    return [experts - sum(sizes)] + sizes


def solution(mesh):
    row_spec = P(('data', 'ep'))

    def device_step(x_in, w_query, w_keyval, w_out, attn_gain, moe_gain, w_gate, w_up, w_down, expert_ids, slot_ids, fill_counts, route_weight):
        batch_loc, seq_len, model_dim = x_in.shape
        rows_loc, num_heads, head_dim = w_query.shape
        q_cols = num_heads * head_dim
        k_cols = w_keyval.shape[1] // 2 * head_dim
        experts = w_gate.shape[0]
        inner = w_gate.shape[2]
        w_local = jnp.concatenate([w_query.reshape(rows_loc, q_cols), w_keyval.reshape(rows_loc, 2 * k_cols), w_out], axis=1)
        attn_blocks = w_local.shape[1] // inner
        mats = (w_gate, w_up, jnp.swapaxes(w_down, 1, 2))
        stacks = []
        first = 0
        for size in shares_of(experts):
            stacks.append([mat[first:first + size] for mat in mats])
            first += size
        stacks[0] = [w_local[None, :, i * inner:(i + 1) * inner] for i in range(attn_blocks)] + stacks[0]
        stacks = [jnp.concatenate(stack) for stack in stacks]
        head = lax.all_gather(stacks[0], 'ep', axis=0, tiled=False)
        tables = rotary_tables(seq_len, head_dim)
        routing = [routing_tables(expert_ids[b], slot_ids[b], fill_counts[0], route_weight[b]) for b in range(batch_loc)]
        gains = (attn_gain[None, :], moe_gain[None, :])
        stacks, tables, routing, gains, head = lax.optimization_barrier((stacks[1:], tables, routing, gains, head))
        parts = [head] + [lax.all_gather(part, 'ep', axis=0, tiled=False) for part in stacks]
        outs = []
        for b in range(batch_loc):
            outs.append(local_layer(x_in[b], *gains, parts, attn_blocks, routing[b], tables, head_dim, q_cols, k_cols))
        return jnp.stack(outs)

    in_specs = (row_spec, P('ep'), P('ep'), P('ep'), P(), P(), P(None, 'ep'), P(None, 'ep'), P(None, None, 'ep'), row_spec, row_spec, row_spec, row_spec)
    return jax.shard_map(device_step, mesh=mesh, in_specs=in_specs, out_specs=row_spec, check_vma=False)
```
